128 devices in a mesh: rep: 2 (over core), dp: 64 (over x, y, z).
Axes of the slice: x: 4, y: 4, z: 4, core: 2. Of those that a mesh axis runs over, the one named last changes fastest.
Arguments:
- g_w_gate: bfloat16 [128, 2, 512, 8192], P(('rep', 'dp')), parts along dimension 0
- g_w_up: bfloat16 [128, 2, 512, 8192], P(('rep', 'dp')), parts along dimension 0
- g_w_down: bfloat16 [128, 2, 8192, 512], P(('rep', 'dp')), parts along dimension 0
- w_gate: bfloat16 [2, 512, 8192], replicated
- w_up: bfloat16 [2, 512, 8192], replicated
- w_down: bfloat16 [2, 8192, 512], replicated
- m_w_gate: float32 [2, 512, 8192], P(None, 'dp')
- m_w_up: float32 [2, 512, 8192], P(None, 'dp')
- m_w_down: float32 [2, 8192, 512], P(None, 'dp')
- v_w_gate: float32 [2, 512, 8192], P(None, 'dp')
- v_w_up: float32 [2, 512, 8192], P(None, 'dp')
- v_w_down: float32 [2, 8192, 512], P(None, 'dp')
Outputs:
- output 1: bfloat16 [4, 512, 8192], P('rep'), parts along dimension 0
- output 2: bfloat16 [4, 512, 8192], P('rep'), parts along dimension 0
- output 3: bfloat16 [4, 8192, 512], P('rep'), parts along dimension 0
- output 4: float32 [4, 512, 8192], P('rep', 'dp'), parts along dimension 0
- output 5: float32 [4, 512, 8192], P('rep', 'dp'), parts along dimension 0
- output 6: float32 [4, 8192, 512], P('rep', 'dp'), parts along dimension 0
- output 7: float32 [4, 512, 8192], P('rep', 'dp'), parts along dimension 0
- output 8: float32 [4, 512, 8192], P('rep', 'dp'), parts along dimension 0
- output 9: float32 [4, 8192, 512], P('rep', 'dp'), parts along dimension 0
There are 2 independent parts. The reference program is written for one: setup_inputs(seed, part) draws one part's arguments, and reference() takes and returns one part's arrays. A program takes and returns all parts, laid end to end along the dimension named above; an argument that names none is the same for every part.
All inputs are finite; a program needn't handle non-finite values.
Results may differ from the reference program's by a relative error of at most 0.022.
Values are sent between devices in bfloat16 or wider.
A program may use at most 1.5 GiB of HBM per device.

```python
import jax
import jax.numpy as jnp
from jax import lax

DEVICES = 64
D = 512
FF = 8192
LAYERS = 2
NAMES = ("w_gate", "w_up", "w_down")
SHAPES = {"w_gate": (LAYERS, D, FF), "w_up": (LAYERS, D, FF), "w_down": (LAYERS, FF, D)}


def setup_inputs(seed: int = 0, part: int = 0) -> dict:
    kz, *keys = jax.random.split(jax.random.key(seed), 1 + 5 * len(NAMES))
    loud = 2.0 ** jax.random.uniform(kz, (), jnp.float32, -1.0, 1.0)
    drawn = {}
    for name, key, both in zip(NAMES, keys[:3], keys[3:6], strict=True):
        own = jax.random.normal(jax.random.fold_in(key, part), (DEVICES, *SHAPES[name]), jnp.float32)
        shared = jax.random.normal(jax.random.fold_in(both, part), SHAPES[name], jnp.float32)
        drawn["g_" + name] = (loud * (0.7 * shared / DEVICES + 0.7 * own * DEVICES**-0.5)).astype(jnp.bfloat16)
    for name, key in zip(NAMES, keys[6:9], strict=True):
        drawn[name] = (jax.random.normal(key, SHAPES[name], jnp.float32) * SHAPES[name][1] ** -0.5).astype(jnp.bfloat16)
    for name, key in zip(NAMES, keys[9:12], strict=True):
        drawn["m_" + name] = loud * 0.5 * jax.random.normal(key, SHAPES[name], jnp.float32)
    for name, key in zip(NAMES, keys[12:15], strict=True):
        drawn["v_" + name] = loud * loud * jax.random.uniform(key, SHAPES[name], jnp.float32, 0.5, 1.5)
    return drawn


def adamw(w, m, v, g):
    m = 0.9 * m + 0.1 * g
    v = 0.95 * v + 0.05 * g * g
    step = m * lax.rsqrt(v + 1e-8) + 0.1 * w
    return (w - 0.02 * step).astype(jnp.bfloat16), m, v


def clipped(gradients, sum_of_squares, count):
    factor = jnp.minimum(1.0, 0.5 * lax.rsqrt(sum_of_squares / count + 1e-30))
    return [g * factor for g in gradients]


def reference(g_w_gate, g_w_up, g_w_down, w_gate, w_up, w_down, m_w_gate, m_w_up, m_w_down, v_w_gate, v_w_up, v_w_down):
    def total(terms):
        return lax.scan(lambda so_far, term: (so_far + term.astype(jnp.float32), None), jnp.zeros(terms.shape[1:], jnp.float32), terms)[0]

    gradients = [total(terms).astype(jnp.bfloat16).astype(jnp.float32) for terms in (g_w_gate, g_w_up, g_w_down)]
    gradients = clipped(gradients, sum(jnp.sum(g * g) for g in gradients), sum(g.size for g in gradients))
    new = [
        adamw(w.astype(jnp.float32), m, v, g)
        for w, m, v, g in zip((w_gate, w_up, w_down), (m_w_gate, m_w_up, m_w_down), (v_w_gate, v_w_up, v_w_down), gradients, strict=True)
    ]
    return tuple(one[which] for which in range(3) for one in new)
```

```python
import functools

import jax
import jax.numpy as jnp
from jax import lax
from jax.experimental import pallas as pl
from jax.experimental.pallas import tpu as pltpu
from jax.sharding import PartitionSpec as P

MESH = pl.DeviceIdType.MESH
RING = 4
STRIDE = (16, 4, 1)
ORDERS = ((0, 1, 2), (1, 2, 0), (2, 0, 1))
SLOTS = 4
FAR, NEAR, SUM = 0, 1, 2
KEEP_UP, KEEP_DOWN, OWN = 0, 1, 2


def adamw(w, m, v, g):
    m = 0.9 * m + 0.1 * g
    v = 0.95 * v + 0.05 * g * g
    step = m * lax.rsqrt(v + 1e-8) + 0.1 * w
    return (w - 0.02 * step).astype(jnp.bfloat16), m, v


def tiles_of(a):
    layers, rows, columns = a.shape
    a = a.reshape(layers, rows // 8, 8, columns // 128, 128).transpose(0, 1, 3, 2, 4)
    return a.reshape(layers, rows // 8 * columns // 128, 8, 128)


def from_tiles(a, rows, columns):
    a = a.reshape(a.shape[0], rows // 8, columns // 128, 8, 128).transpose(0, 1, 3, 2, 4)
    return a.reshape(a.shape[0], rows, columns)


class Here:
    def __init__(self):
        self.index = lax.axis_index("dp")
        self.coords = tuple(lax.rem(lax.div(self.index, stride), RING) for stride in STRIDE)

    def coord(self, axis, offset):
        return lax.rem(self.coords[axis] + (offset + RING), RING)

    def peer(self, axis, offset):
        return {"dp": self.index + (self.coord(axis, offset) - self.coords[axis]) * STRIDE[axis]}

    def meet(self, offsets):
        barrier = pltpu.get_barrier_semaphore()
        for axis in range(3):
            for offset in offsets:
                pl.semaphore_signal(barrier, inc=1, device_id=self.peer(axis, offset), device_id_type=MESH)
        pl.semaphore_wait(barrier, 3 * len(offsets))


def sum_kernel(chunks, tiles, *refs):
    terms, (total, squares), scratch = refs[:3], refs[3:5], refs[5:]
    (stage, recv, sums, outs, keep, acc, norms), (sent, got, staged, credit, norm_sent, norm_got) = scratch
    here = Here()
    here.meet((1, -1, 2))
    steps = chunks + 6

    def part(i, axis, half, offset, k):
        index = [slice(None)] * 3
        index[axis] = here.coord(axis, offset)
        return terms[i].at[(half, *index, pl.ds(k * tiles, tiles))]

    def message(p, k, i, s, kind):
        axis, slot = ORDERS[i][p], lax.rem(k, SLOTS)
        if kind == SUM:
            source = sums[p].at[i, s, slot]
        elif p:
            source = outs[p].at[i, s, kind, slot]
        elif kind == FAR:
            source = part(i, axis, s, 2, k)
        else:
            source = part(i, axis, 1 - s, (1, -1)[s], k)
        return pltpu.make_async_remote_copy(
            source,
            recv[p].at[i, s, kind, slot],
            sent.at[p, i, s, kind, slot],
            got.at[p, i, s, kind, slot],
            device_id=here.peer(axis, (1, -1)[s]),
            device_id_type=MESH,
        )

    def staging(k, i, what):
        axis, slot = ORDERS[i][0], lax.rem(k, SLOTS)
        half, offset = ((0, 1), (1, -1), (0, 0), (1, 0))[what]
        return pltpu.make_async_copy(part(i, axis, half, offset, k), stage.at[i, what, slot], staged.at[i, what, slot])

    def start(p, k, kinds):
        for kind in kinds:
            for i in range(3):
                for s in range(2):
                    message(p, k, i, s, kind).start()

    def reuse(p, k, kinds):
        @pl.when(k >= SLOTS)
        def _():
            for kind in kinds:
                for i in range(3):
                    for s in range(2):
                        message(p, k - SLOTS, i, s, kind).wait_send()

    def first(k):
        reuse(0, k, (FAR, NEAR))
        start(0, k, (FAR, NEAR))
        for what in range(4):
            for i in range(3):
                staging(k, i, what).start()

    def held(p, i, what, slot, index):
        if p:
            return keep[p][(i, what, slot, *index)]
        return stage[(i, what, slot, *index)].astype(jnp.float32)

    def middle(p, k):
        slot = lax.rem(k, SLOTS)
        reuse(p, k, (SUM,))
        for i in range(3):
            for s in range(2):
                message(p, k, i, s, FAR).wait_recv()
                if p == 0:
                    staging(k, i, s).wait()

                def add(index):
                    whole = held(p, i, s, slot, index) + recv[p][(i, s, FAR, slot, *index)].astype(jnp.float32)
                    sums[p][(i, s, slot, *index)] = whole.astype(jnp.bfloat16)

                if p == 0:
                    pl.loop(0, RING * RING)(lambda j: add((lax.div(j, RING), lax.rem(j, RING))))
                elif p == 1:
                    pl.loop(0, RING)(lambda j: add((j,)))
                else:
                    add(())
        start(p, k, (SUM,))

    def last(p, k):
        slot = lax.rem(k, SLOTS)
        if p < 2:
            reuse(p + 1, k, (FAR, NEAR))
        for i in range(3):
            for s in range(2):
                message(p, k, i, s, SUM).wait_recv()
                message(p, k, i, s, NEAR).wait_recv()
                if p == 0:
                    staging(k, i, OWN + s).wait()

            def whole(half, index):
                return (
                    held(p, i, OWN + half, slot, index)
                    + recv[p][(i, half, SUM, slot, *index)].astype(jnp.float32)
                    + recv[p][(i, 1 - half, NEAR, slot, *index)].astype(jnp.float32)
                )

            if p == 2:
                for half in range(2):
                    g = whole(half, ()).astype(jnp.bfloat16)
                    total[i, half, pl.ds(k * tiles, tiles)] = g
                    g = g.astype(jnp.float32)
                    acc[...] += jnp.sum(g * g, axis=0)
                continue
            axis = ORDERS[i][p + 1]

            def pass_on(below):
                for half in range(2):
                    for offset in range(RING):
                        at = here.coord(axis, offset)
                        if p == 1:
                            index = (at,)
                        elif axis > ORDERS[i][2]:
                            index = (below, at)
                        else:
                            index = (at, below)
                        value = whole(half, index)
                        to = () if p == 1 else (below,)
                        if offset == 0:
                            keep[p + 1][(i, OWN + half, slot, *to)] = value
                        elif offset == (1, 3)[half]:
                            keep[p + 1][(i, half, slot, *to)] = value
                        elif offset == 2:
                            outs[p + 1][(i, half, FAR, slot, *to)] = value.astype(jnp.bfloat16)
                        else:
                            outs[p + 1][(i, 1 - half, NEAR, slot, *to)] = value.astype(jnp.bfloat16)

            if p == 0:
                pl.loop(0, RING)(pass_on)
            else:
                pass_on(None)
        if p < 2:
            start(p + 1, k, (FAR, NEAR))

    acc[...] = jnp.zeros_like(acc)

    @pl.loop(0, steps)
    def _(n):
        @pl.when(n >= 2)
        def _():
            for to in range(6):
                pl.semaphore_wait(credit.at[to], 1)

        for late, work in enumerate(
            (
                first,
                functools.partial(middle, 0),
                functools.partial(last, 0),
                functools.partial(middle, 1),
                functools.partial(last, 1),
                functools.partial(middle, 2),
                functools.partial(last, 2),
            )
        ):
            k = n - late
            pl.when(jnp.logical_and(k >= 0, k < chunks))(functools.partial(work, k))

        @pl.when(n < steps - 2)
        def _():
            for axis in range(3):
                for s in range(2):
                    pl.semaphore_signal(credit.at[2 * axis + 1 - s], inc=1, device_id=here.peer(axis, (1, -1)[s]), device_id_type=MESH)

    for p in range(3):
        for k in range(chunks - SLOTS, chunks):
            for kind in range(3):
                for i in range(3):
                    for s in range(2):
                        message(p, k, i, s, kind).wait_send()

    for axis in range(3):
        mine = here.coords[axis]
        norms[axis, mine] = acc[...]
        copies = [
            pltpu.make_async_remote_copy(
                norms.at[axis, mine],
                norms.at[axis, mine],
                norm_sent.at[axis, offset],
                norm_got.at[axis, offset],
                device_id=here.peer(axis, offset + 1),
                device_id_type=MESH,
            )
            for offset in range(3)
        ]
        for copy in copies:
            copy.start()
        for copy in copies:
            copy.wait()
        acc[...] = norms[axis, 0] + norms[axis, 1] + norms[axis, 2] + norms[axis, 3]
    squares[...] = acc[...]


def sum_scatter(terms, chunks):
    count = terms[0].shape[4]
    tiles = count // chunks
    dma, bf16, f32 = pltpu.SemaphoreType.DMA, jnp.bfloat16, jnp.float32
    subs = ((RING, RING), (RING,), ())
    tile = (tiles, 8, 128)
    per = range(3)
    buffers = (
        pltpu.VMEM((3, 4, SLOTS, *subs[0], *tile), bf16),
        [pltpu.VMEM((3, 2, 3, SLOTS, *subs[p], *tile), bf16) for p in per],
        [pltpu.VMEM((3, 2, SLOTS, *subs[p], *tile), bf16) for p in per],
        [pltpu.VMEM((3, 2, 2, SLOTS, *subs[p], *tile) if p else (8, 128), bf16) for p in per],
        [pltpu.VMEM((3, 4, SLOTS, *subs[p], *tile) if p else (8, 128), f32) for p in per],
        pltpu.VMEM((8, 128), f32),
        pltpu.VMEM((3, RING, 8, 128), f32),
    )
    semaphores = (
        dma((3, 3, 2, 3, SLOTS)),
        dma((3, 3, 2, 3, SLOTS)),
        dma((3, 4, SLOTS)),
        pltpu.SemaphoreType.REGULAR((6,)),
        dma((3, 3)),
        dma((3, 3)),
    )
    return pl.pallas_call(
        functools.partial(sum_kernel, chunks, tiles),
        out_shape=(jax.ShapeDtypeStruct((3, 2, count, 8, 128), bf16), jax.ShapeDtypeStruct((8, 128), f32)),
        in_specs=[pl.BlockSpec(memory_space=pl.ANY)] * 3,
        out_specs=[pl.BlockSpec(memory_space=pltpu.VMEM)] * 2,
        scratch_shapes=[buffers, semaphores],
        compiler_params=pltpu.CompilerParams(collective_id=0, has_side_effects=True, vmem_limit_bytes=60 * 2**20),
        name="sum_scatter",
    )(*terms)


def gather_kernel(chunks, tiles, *refs):
    blocks, wholes, (sent, got, placed) = refs[:3], refs[3:6], refs[6:]
    here = Here()
    here.meet((1, -1))

    def region(i, q, half, offset, k):
        index = list(here.coords)
        for done in range(q):
            index[ORDERS[i][2 - done]] = slice(None)
        axis = ORDERS[i][2 - q]
        index[axis] = here.coord(axis, offset)
        return wholes[i].at[(half, *index, pl.ds(k * tiles, tiles))]

    def message(q, k, i, s, on):
        if on:
            target = region(i, q, s, (-1, 1)[s], k)
        else:
            target = region(i, q, slice(None), 0, k)
        return pltpu.make_async_remote_copy(
            blocks[i].at[:, pl.ds(k * tiles, tiles)] if q == 0 and not on else target,
            target,
            sent.at[q, i, s, on, k],
            got.at[q, i, s, on, k],
            device_id=here.peer(ORDERS[i][2 - q], (1, -1)[s]),
            device_id_type=MESH,
        )

    def each(q, k, on, act):
        for i in range(3):
            for s in range(2):
                act(message(q, k, i, s, on))

    def start(copy):
        copy.start()

    def arrive(copy):
        copy.wait_recv()

    def leave(copy):
        copy.wait_send()

    own = [pltpu.make_async_copy(blocks[i], wholes[i].at[(slice(None), *here.coords)], placed.at[i]) for i in range(3)]
    pl.loop(0, chunks)(lambda k: each(0, k, 0, start))
    for copy in own:
        copy.start()
    for copy in own:
        copy.wait()

    def onward(q, k):
        each(q, k, 0, arrive)
        each(q, k, 1, start)

    def widen(q, k):
        each(q, k, 1, arrive)
        if q < 2:
            each(q + 1, k, 0, start)

    @pl.loop(0, chunks + 5)
    def _(n):
        for late in range(6):
            k = n - late
            work = functools.partial(widen if late % 2 else onward, late // 2, k)
            pl.when(jnp.logical_and(k >= 0, k < chunks))(work)

    @pl.loop(0, chunks)
    def _(k):
        for q in range(3):
            for on in range(2):
                each(q, k, on, leave)


def gather(blocks, chunks):
    count = blocks[0].shape[1]
    tiles = count // chunks
    dma = pltpu.SemaphoreType.DMA
    whole = jax.ShapeDtypeStruct((2, RING, RING, RING, count, 8, 128), jnp.bfloat16)
    return pl.pallas_call(
        functools.partial(gather_kernel, chunks, tiles),
        out_shape=(whole,) * 3,
        in_specs=[pl.BlockSpec(memory_space=pltpu.VMEM)] * 3,
        out_specs=[pl.BlockSpec(memory_space=pl.ANY)] * 3,
        scratch_shapes=[dma((3, 3, 2, 2, chunks)), dma((3, 3, 2, 2, chunks)), dma((3,))],
        compiler_params=pltpu.CompilerParams(collective_id=1, has_side_effects=True),
        name="gather",
    )(*blocks)


def solution(mesh):
    def step(*arrays):
        terms, weights, m, v = (arrays[i : i + 3] for i in (0, 3, 6, 9))
        shapes = [w.shape for w in weights]
        views = [tiles_of(t[0]).reshape(2, RING, RING, RING, -1, 8, 128) for t in terms]
        total, squares = sum_scatter(views, 16)
        count = lax.psum(1, "dp") * sum(one.size for one in m)
        factor = jnp.minimum(1.0, 0.5 * lax.rsqrt(jnp.sum(squares) / count + 1e-30))
        gradients = [from_tiles(total[i], *one.shape[1:]).astype(jnp.float32) * factor for i, one in enumerate(m)]
        me = lax.axis_index("dp")
        own = [lax.dynamic_slice_in_dim(w, me * one.shape[1], one.shape[1], 1).astype(jnp.float32) for w, one in zip(weights, m, strict=True)]
        new = [adamw(w, m, v, g) for w, m, v, g in zip(own, m, v, gradients, strict=True)]
        whole = gather([tiles_of(one[0]) for one in new], 8)
        whole = [from_tiles(one.reshape(2, -1, 8, 128), *shape[1:]) for one, shape in zip(whole, shapes, strict=True)]
        return (*whole, *(one[1] for one in new), *(one[2] for one in new))

    all_of, cut = P(None, None, None), P(None, "dp", None)
    return jax.shard_map(
        step,
        mesh=mesh,
        in_specs=(P(("rep", "dp"), None, None, None),) * 3 + (all_of,) * 3 + (cut,) * 6,
        out_specs=(P("rep", None, None),) * 3 + (P("rep", "dp", None),) * 6,
        check_vma=False,
    )
```

```python
import functools

import jax
import jax.numpy as jnp
from jax import lax
from jax.experimental import pallas as pl
from jax.experimental.pallas import tpu as pltpu
from jax.sharding import PartitionSpec as P

MESH = pl.DeviceIdType.MESH
RING = 4
STRIDE = (16, 4, 1)
ORDERS = ((0, 1, 2), (1, 2, 0), (2, 0, 1))
SLOTS = 4
FAR, NEAR, SUM = 0, 1, 2
KEEP_UP, KEEP_DOWN, OWN = 0, 1, 2


def adamw(w, m, v, g):
    m = 0.9 * m + 0.1 * g
    v = 0.95 * v + 0.05 * g * g
    step = m * lax.rsqrt(v + 1e-8) + 0.1 * w
    return (w - 0.02 * step).astype(jnp.bfloat16), m, v


def tiles_of(a):
    layers, rows, columns = a.shape
    a = a.reshape(layers, rows // 8, 8, columns // 128, 128).transpose(0, 1, 3, 2, 4)
    return a.reshape(layers, rows // 8 * columns // 128, 8, 128)


def from_tiles(a, rows, columns):
    a = a.reshape(a.shape[0], rows // 8, columns // 128, 8, 128).transpose(0, 1, 3, 2, 4)
    return a.reshape(a.shape[0], rows, columns)


class Here:
    def __init__(self):
        self.index = lax.axis_index("dp")
        self.coords = tuple(lax.rem(lax.div(self.index, stride), RING) for stride in STRIDE)

    def coord(self, axis, offset):
        return lax.rem(self.coords[axis] + (offset + RING), RING)

    def peer(self, axis, offset):
        return {"dp": self.index + (self.coord(axis, offset) - self.coords[axis]) * STRIDE[axis]}

    def meet(self, offsets):
        barrier = pltpu.get_barrier_semaphore()
        for axis in range(3):
            for offset in offsets:
                pl.semaphore_signal(barrier, inc=1, device_id=self.peer(axis, offset), device_id_type=MESH)
        pl.semaphore_wait(barrier, 3 * len(offsets))


def sum_kernel(chunks, tiles, *refs):
    terms, (total, squares), scratch = refs[:3], refs[3:5], refs[5:]
    (stage, recv, sums, outs, keep, acc, norms), (sent, got, staged, credit, norm_sent, norm_got) = scratch
    here = Here()
    here.meet((1, -1, 2))
    steps = chunks + 6

    def part(i, axis, half, offset, k):
        index = [slice(None)] * 3
        index[axis] = here.coord(axis, offset)
        return terms[i].at[(half, *index, pl.ds(k * tiles, tiles))]

    def message(p, k, i, s, kind):
        axis, slot = ORDERS[i][p], lax.rem(k, SLOTS)
        if kind == SUM:
            source = sums[p].at[i, s, slot]
        elif p:
            source = outs[p].at[i, s, kind, slot]
        elif kind == FAR:
            source = part(i, axis, s, 2, k)
        else:
            source = part(i, axis, 1 - s, (1, -1)[s], k)
        return pltpu.make_async_remote_copy(
            source,
            recv[p].at[i, s, kind, slot],
            sent.at[p, i, s, kind, slot],
            got.at[p, i, s, kind, slot],
            device_id=here.peer(axis, (1, -1)[s]),
            device_id_type=MESH,
        )

    def staging(k, i, what):
        axis, slot = ORDERS[i][0], lax.rem(k, SLOTS)
        half, offset = ((0, 1), (1, -1), (0, 0), (1, 0))[what]
        return pltpu.make_async_copy(part(i, axis, half, offset, k), stage.at[i, what, slot], staged.at[i, what, slot])

    def start(p, k, kinds):
        for kind in kinds:
            for i in range(3):
                for s in range(2):
                    message(p, k, i, s, kind).start()

    def reuse(p, k, kinds):
        @pl.when(k >= SLOTS)
        def _():
            for kind in kinds:
                for i in range(3):
                    for s in range(2):
                        message(p, k - SLOTS, i, s, kind).wait_send()

    def first(k):
        reuse(0, k, (FAR, NEAR))
        start(0, k, (FAR, NEAR))
        for what in range(4):
            for i in range(3):
                staging(k, i, what).start()

    def held(p, i, what, slot, index):
        if p:
            return keep[p][(i, what, slot, *index)]
        return stage[(i, what, slot, *index)].astype(jnp.float32)

    def middle(p, k):
        slot = lax.rem(k, SLOTS)
        reuse(p, k, (SUM,))
        for i in range(3):
            for s in range(2):
                message(p, k, i, s, FAR).wait_recv()
                if p == 0:
                    staging(k, i, s).wait()

                def add(index):
                    whole = held(p, i, s, slot, index) + recv[p][(i, s, FAR, slot, *index)].astype(jnp.float32)
                    sums[p][(i, s, slot, *index)] = whole.astype(jnp.bfloat16)

                if p == 0:
                    pl.loop(0, RING * RING)(lambda j: add((lax.div(j, RING), lax.rem(j, RING))))
                elif p == 1:
                    pl.loop(0, RING)(lambda j: add((j,)))
                else:
                    add(())
        start(p, k, (SUM,))

    def last(p, k):
        slot = lax.rem(k, SLOTS)
        if p < 2:
            reuse(p + 1, k, (FAR, NEAR))
        for i in range(3):
            for s in range(2):
                message(p, k, i, s, SUM).wait_recv()
                message(p, k, i, s, NEAR).wait_recv()
                if p == 0:
                    staging(k, i, OWN + s).wait()

            def whole(half, index):
                return (
                    held(p, i, OWN + half, slot, index)
                    + recv[p][(i, half, SUM, slot, *index)].astype(jnp.float32)
                    + recv[p][(i, 1 - half, NEAR, slot, *index)].astype(jnp.float32)
                )

            if p == 2:
                for half in range(2):
                    g = whole(half, ()).astype(jnp.bfloat16)
                    total[i, half, pl.ds(k * tiles, tiles)] = g
                    g = g.astype(jnp.float32)
                    acc[...] += jnp.sum(g * g, axis=0)
                continue
            axis = ORDERS[i][p + 1]

            def pass_on(below):
                for half in range(2):
                    for offset in range(RING):
                        at = here.coord(axis, offset)
                        if p == 1:
                            index = (at,)
                        elif axis > ORDERS[i][2]:
                            index = (below, at)
                        else:
                            index = (at, below)
                        value = whole(half, index)
                        to = () if p == 1 else (below,)
                        if offset == 0:
                            keep[p + 1][(i, OWN + half, slot, *to)] = value
                        elif offset == (1, 3)[half]:
                            keep[p + 1][(i, half, slot, *to)] = value
                        elif offset == 2:
                            outs[p + 1][(i, half, FAR, slot, *to)] = value.astype(jnp.bfloat16)
                        else:
                            outs[p + 1][(i, 1 - half, NEAR, slot, *to)] = value.astype(jnp.bfloat16)

            if p == 0:
                pl.loop(0, RING)(pass_on)
            else:
                pass_on(None)
        if p < 2:
            start(p + 1, k, (FAR, NEAR))

    acc[...] = jnp.zeros_like(acc)

    @pl.loop(0, steps)
    def _(n):
        @pl.when(n >= 2)
        def _():
            for to in range(6):
                pl.semaphore_wait(credit.at[to], 1)

        for late, work in enumerate(
            (
                first,
                functools.partial(middle, 0),
                functools.partial(last, 0),
                functools.partial(middle, 1),
                functools.partial(last, 1),
                functools.partial(middle, 2),
                functools.partial(last, 2),
            )
        ):
            k = n - late
            pl.when(jnp.logical_and(k >= 0, k < chunks))(functools.partial(work, k))

        @pl.when(n < steps - 2)
        def _():
            for axis in range(3):
                for s in range(2):
                    pl.semaphore_signal(credit.at[2 * axis + 1 - s], inc=1, device_id=here.peer(axis, (1, -1)[s]), device_id_type=MESH)

    for p in range(3):
        for k in range(chunks - SLOTS, chunks):
            for kind in range(3):
                for i in range(3):
                    for s in range(2):
                        message(p, k, i, s, kind).wait_send()

    for axis in range(3):
        mine = here.coords[axis]
        norms[axis, mine] = acc[...]
        copies = [
            pltpu.make_async_remote_copy(
                norms.at[axis, mine],
                norms.at[axis, mine],
                norm_sent.at[axis, offset],
                norm_got.at[axis, offset],
                device_id=here.peer(axis, offset + 1),
                device_id_type=MESH,
            )
            for offset in range(3)
        ]
        for copy in copies:
            copy.start()
        for copy in copies:
            copy.wait()
        acc[...] = norms[axis, 0] + norms[axis, 1] + norms[axis, 2] + norms[axis, 3]
    squares[...] = acc[...]


def sum_scatter(terms, chunks):
    count = terms[0].shape[4]
    tiles = count // chunks
    dma, bf16, f32 = pltpu.SemaphoreType.DMA, jnp.bfloat16, jnp.float32
    subs = ((RING, RING), (RING,), ())
    tile = (tiles, 8, 128)
    per = range(3)
    buffers = (
        pltpu.VMEM((3, 4, SLOTS, *subs[0], *tile), bf16),
        [pltpu.VMEM((3, 2, 3, SLOTS, *subs[p], *tile), bf16) for p in per],
        [pltpu.VMEM((3, 2, SLOTS, *subs[p], *tile), bf16) for p in per],
        [pltpu.VMEM((3, 2, 2, SLOTS, *subs[p], *tile) if p else (8, 128), bf16) for p in per],
        [pltpu.VMEM((3, 4, SLOTS, *subs[p], *tile) if p else (8, 128), f32) for p in per],
        pltpu.VMEM((8, 128), f32),
        pltpu.VMEM((3, RING, 8, 128), f32),
    )
    semaphores = (
        dma((3, 3, 2, 3, SLOTS)),
        dma((3, 3, 2, 3, SLOTS)),
        dma((3, 4, SLOTS)),
        pltpu.SemaphoreType.REGULAR((6,)),
        dma((3, 3)),
        dma((3, 3)),
    )
    return pl.pallas_call(
        functools.partial(sum_kernel, chunks, tiles),
        out_shape=(jax.ShapeDtypeStruct((3, 2, count, 8, 128), bf16), jax.ShapeDtypeStruct((8, 128), f32)),
        in_specs=[pl.BlockSpec(memory_space=pl.ANY)] * 3,
        out_specs=[pl.BlockSpec(memory_space=pltpu.VMEM)] * 2,
        scratch_shapes=[buffers, semaphores],
        compiler_params=pltpu.CompilerParams(collective_id=0, has_side_effects=True, vmem_limit_bytes=60 * 2**20),
        name="sum_scatter",
    )(*terms)


def gather_kernel(chunks, tiles, *refs):
    blocks, wholes, (sent, got) = refs[:3], [refs[3].at[i] for i in range(3)], refs[4:]
    here = Here()
    here.meet((1, -1))

    def region(i, q, half, offset, k):
        index = list(here.coords)
        for done in range(q):
            index[ORDERS[i][2 - done]] = slice(None)
        axis = ORDERS[i][2 - q]
        index[axis] = here.coord(axis, offset)
        return wholes[i].at[(half, *index, pl.ds(k * tiles, tiles))]

    def message(q, k, i, s, on):
        if on:
            target = region(i, q, s, (-1, 1)[s], k)
        else:
            target = region(i, q, slice(None), 0, k)
        return pltpu.make_async_remote_copy(
            blocks[i].at[:, pl.ds(k * tiles, tiles)] if q == 0 and not on else target,
            target,
            sent.at[q, i, s, on, k],
            got.at[q, i, s, on, k],
            device_id=here.peer(ORDERS[i][2 - q], (1, -1)[s]),
            device_id_type=MESH,
        )

    def each(q, k, on, act):
        for i in range(3):
            for s in range(2):
                act(message(q, k, i, s, on))

    def start(copy):
        copy.start()

    def arrive(copy):
        copy.wait_recv()

    def leave(copy):
        copy.wait_send()

    pl.loop(0, chunks)(lambda k: each(0, k, 0, start))

    @pl.loop(0, chunks)
    def _(k):
        for i in range(3):
            for half in range(2):
                some = pl.ds(k * tiles, tiles)
                wholes[i][(half, *here.coords, some)] = blocks[i][half, some]

    def onward(q, k):
        each(q, k, 0, arrive)
        each(q, k, 1, start)

    def widen(q, k):
        each(q, k, 1, arrive)
        if q < 2:
            each(q + 1, k, 0, start)

    @pl.loop(0, chunks + 5)
    def _(n):
        for late in range(6):
            k = n - late
            work = functools.partial(widen if late % 2 else onward, late // 2, k)
            pl.when(jnp.logical_and(k >= 0, k < chunks))(work)

    @pl.loop(0, chunks)
    def _(k):
        for q in range(3):
            for on in range(2):
                each(q, k, on, leave)


def write_kernel(*refs):
    wholes, outs, done = [refs[0].at[i] for i in range(3)], refs[1:4], refs[4]
    copies = [
        pltpu.make_async_copy(wholes[i].at[half, x], outs[i].at[half, x], done.at[i, half, x])
        for i in range(3)
        for half in range(2)
        for x in range(RING)
    ]
    for copy in copies:
        copy.start()
    for copy in copies:
        copy.wait()


def gather(blocks, chunks):
    count = blocks[0].shape[1]
    tiles = count // chunks
    dma = pltpu.SemaphoreType.DMA
    shape = (2, RING, RING, RING, count, 8, 128)
    whole = pl.pallas_call(
        functools.partial(gather_kernel, chunks, tiles),
        out_shape=pltpu.VMEM((3, *shape), jnp.bfloat16),
        in_specs=[pl.BlockSpec(memory_space=pltpu.VMEM)] * 3,
        out_specs=pl.BlockSpec(memory_space=pltpu.VMEM),
        scratch_shapes=[dma((3, 3, 2, 2, chunks)), dma((3, 3, 2, 2, chunks))],
        compiler_params=pltpu.CompilerParams(collective_id=1, has_side_effects=True, vmem_limit_bytes=4 * 2**20),
        name="gather",
    )(*blocks)
    return pl.pallas_call(
        write_kernel,
        out_shape=(jax.ShapeDtypeStruct(shape, jnp.bfloat16),) * 3,
        in_specs=[pl.BlockSpec(memory_space=pltpu.VMEM)],
        out_specs=[pl.BlockSpec(memory_space=pl.ANY)] * 3,
        scratch_shapes=[dma((3, 2, RING))],
        compiler_params=pltpu.CompilerParams(has_side_effects=True, vmem_limit_bytes=4 * 2**20),
        name="write",
    )(whole)


def solution(mesh):
    def step(*arrays):
        terms, weights, m, v = (arrays[i : i + 3] for i in (0, 3, 6, 9))
        shapes = [w.shape for w in weights]
        views = [tiles_of(t[0]).reshape(2, RING, RING, RING, -1, 8, 128) for t in terms]
        total, squares = sum_scatter(views, 16)
        count = lax.psum(1, "dp") * sum(one.size for one in m)
        factor = jnp.minimum(1.0, 0.5 * lax.rsqrt(jnp.sum(squares) / count + 1e-30))
        gradients = [from_tiles(total[i], *one.shape[1:]).astype(jnp.float32) * factor for i, one in enumerate(m)]
        me = lax.axis_index("dp")
        own = [lax.dynamic_slice_in_dim(w, me * one.shape[1], one.shape[1], 1).astype(jnp.float32) for w, one in zip(weights, m, strict=True)]
        new = [adamw(w, m, v, g) for w, m, v, g in zip(own, m, v, gradients, strict=True)]
        whole = gather([tiles_of(one[0]) for one in new], 8)
        whole = [from_tiles(one.reshape(2, -1, 8, 128), *shape[1:]) for one, shape in zip(whole, shapes, strict=True)]
        return (*whole, *(one[1] for one in new), *(one[2] for one in new))

    all_of, cut = P(None, None, None), P(None, "dp", None)
    return jax.shard_map(
        step,
        mesh=mesh,
        in_specs=(P(("rep", "dp"), None, None, None),) * 3 + (all_of,) * 3 + (cut,) * 6,
        out_specs=(P("rep", None, None),) * 3 + (P("rep", "dp", None),) * 6,
        check_vma=False,
    )
```

```python
import functools

import jax
import jax.numpy as jnp
from jax import lax
from jax.experimental import pallas as pl
from jax.experimental.pallas import tpu as pltpu
from jax.sharding import PartitionSpec as P

MESH = pl.DeviceIdType.MESH
RING = 4
STRIDE = (16, 4, 1)
ORDERS = ((0, 1, 2), (1, 2, 0), (2, 0, 1))
SLOTS = 4
STAGES = 5
FAR, NEAR, SUM = 0, 1, 2
KEEP_UP, KEEP_DOWN, OWN = 0, 1, 2


def adamw(w, m, v, g):
    m = 0.9 * m + 0.1 * g
    v = 0.95 * v + 0.05 * g * g
    step = m * lax.rsqrt(v + 1e-8) + 0.1 * w
    return (w - 0.02 * step).astype(jnp.bfloat16), m, v


def tiles_of(a):
    layers, rows, columns = a.shape
    a = a.reshape(layers, rows // 8, 8, columns // 128, 128).transpose(0, 1, 3, 2, 4)
    return a.reshape(layers, rows // 8 * columns // 128, 8, 128)


def from_tiles(a, rows, columns):
    a = a.reshape(a.shape[0], rows // 8, columns // 128, 8, 128).transpose(0, 1, 3, 2, 4)
    return a.reshape(a.shape[0], rows, columns)


class Here:
    def __init__(self):
        self.index = lax.axis_index("dp")
        self.coords = tuple(lax.rem(lax.div(self.index, stride), RING) for stride in STRIDE)

    def coord(self, axis, offset):
        return lax.rem(self.coords[axis] + (offset + RING), RING)

    def peer(self, axis, offset):
        return {"dp": self.index + (self.coord(axis, offset) - self.coords[axis]) * STRIDE[axis]}

    def meet(self, offsets):
        barrier = pltpu.get_barrier_semaphore()
        for axis in range(3):
            for offset in offsets:
                pl.semaphore_signal(barrier, inc=1, device_id=self.peer(axis, offset), device_id_type=MESH)
        pl.semaphore_wait(barrier, 3 * len(offsets))


def sum_kernel(chunks, tiles, *refs):
    terms, weights, old, (new, *moments), scratch = refs[:3], refs[3:6], refs[6:12], refs[12:15], refs[15:]
    (stage, recv, sums, outs, keep, total, own, acc, norms), (sent, got, staged, credit, norm_sent, norm_got, loaded) = scratch
    here = Here()
    steps = chunks + 6

    def part(i, half, offset, k, rest):
        axis = ORDERS[i][0]
        index = (*rest[:axis], here.coord(axis, offset), *rest[axis:])
        return (i, lax.rem(k, STAGES), half, *index)

    everything = (slice(None),) * 2

    def message(p, k, i, s, kind):
        axis, slot = ORDERS[i][p], lax.rem(k, SLOTS)
        if kind == SUM:
            source = sums[p].at[i, s, slot]
        elif p:
            source = outs[p].at[i, s, kind, slot]
        elif kind == FAR:
            source = stage.at[part(i, s, 2, k, everything)]
        else:
            source = stage.at[part(i, 1 - s, (1, -1)[s], k, everything)]
        return pltpu.make_async_remote_copy(
            source,
            recv[p].at[i, s, kind, slot],
            sent.at[p, i, s, kind, slot],
            got.at[p, i, s, kind, slot],
            device_id=here.peer(axis, (1, -1)[s]),
            device_id_type=MESH,
        )

    def staging(k, i):
        slot = lax.rem(k, STAGES)
        source = terms[i].at[:, :, :, :, pl.ds(k * tiles, tiles)]
        return pltpu.make_async_copy(source, stage.at[i, slot], staged.at[i, slot])

    loads = []
    for i in range(3):
        loads.append(pltpu.make_async_copy(weights[i].at[(slice(None), *here.coords)], own.at[i], loaded.at[i, 0]))
        for which in range(2):
            loads.append(pltpu.make_async_copy(old[3 * which + i], moments[which].at[i], loaded.at[i, 1 + which]))
    for i in range(3):
        staging(0, i).start()
    for load in loads:
        load.start()
    here.meet((1, -1, 2))

    def start(p, k, kinds):
        for kind in kinds:
            for i in range(3):
                for s in range(2):
                    message(p, k, i, s, kind).start()

    def reuse(p, k, kinds):
        @pl.when(k >= SLOTS)
        def _():
            for kind in kinds:
                for i in range(3):
                    for s in range(2):
                        message(p, k - SLOTS, i, s, kind).wait_send()

    def first(k):
        reuse(0, k, (FAR, NEAR))
        for i in range(3):
            staging(k, i).wait()
        start(0, k, (FAR, NEAR))

        @pl.when(k + 1 < chunks)
        def _():
            for i in range(3):
                staging(k + 1, i).start()

    def held(p, i, what, k, index):
        if p:
            return keep[p][(i, what, lax.rem(k, SLOTS), *index)]
        half, offset = ((0, 1), (1, -1), (0, 0), (1, 0))[what]
        return stage[part(i, half, offset, k, index)].astype(jnp.float32)

    def middle(p, k):
        slot = lax.rem(k, SLOTS)
        reuse(p, k, (SUM,))
        for i in range(3):
            for s in range(2):
                message(p, k, i, s, FAR).wait_recv()

                def add(index):
                    whole = held(p, i, s, k, index) + recv[p][(i, s, FAR, slot, *index)].astype(jnp.float32)
                    sums[p][(i, s, slot, *index)] = whole.astype(jnp.bfloat16)

                if p == 0:
                    pl.loop(0, RING * RING)(lambda j: add((lax.div(j, RING), lax.rem(j, RING))))
                elif p == 1:
                    pl.loop(0, RING)(lambda j: add((j,)))
                else:
                    add(())
        start(p, k, (SUM,))

    def last(p, k):
        slot = lax.rem(k, SLOTS)
        if p < 2:
            reuse(p + 1, k, (FAR, NEAR))
        for i in range(3):
            for s in range(2):
                message(p, k, i, s, SUM).wait_recv()
                message(p, k, i, s, NEAR).wait_recv()

            def whole(half, index):
                return (
                    held(p, i, OWN + half, k, index)
                    + recv[p][(i, half, SUM, slot, *index)].astype(jnp.float32)
                    + recv[p][(i, 1 - half, NEAR, slot, *index)].astype(jnp.float32)
                )

            if p == 2:
                for half in range(2):
                    g = whole(half, ()).astype(jnp.bfloat16)
                    total[i, half, pl.ds(k * tiles, tiles)] = g
                    g = g.astype(jnp.float32)
                    acc[...] += jnp.sum(g * g, axis=0)
                continue
            axis = ORDERS[i][p + 1]

            def pass_on(below):
                for half in range(2):
                    for offset in range(RING):
                        at = here.coord(axis, offset)
                        if p == 1:
                            index = (at,)
                        elif axis > ORDERS[i][2]:
                            index = (below, at)
                        else:
                            index = (at, below)
                        value = whole(half, index)
                        to = () if p == 1 else (below,)
                        if offset == 0:
                            keep[p + 1][(i, OWN + half, slot, *to)] = value
                        elif offset == (1, 3)[half]:
                            keep[p + 1][(i, half, slot, *to)] = value
                        elif offset == 2:
                            outs[p + 1][(i, half, FAR, slot, *to)] = value.astype(jnp.bfloat16)
                        else:
                            outs[p + 1][(i, 1 - half, NEAR, slot, *to)] = value.astype(jnp.bfloat16)

            if p == 0:
                pl.loop(0, RING)(pass_on)
            else:
                pass_on(None)
        if p < 2:
            start(p + 1, k, (FAR, NEAR))

    acc[...] = jnp.zeros_like(acc)

    @pl.loop(0, steps)
    def _(n):
        @pl.when(n >= 2)
        def _():
            for to in range(6):
                pl.semaphore_wait(credit.at[to], 1)

        for late, work in enumerate(
            (
                first,
                functools.partial(middle, 0),
                functools.partial(last, 0),
                functools.partial(middle, 1),
                functools.partial(last, 1),
                functools.partial(middle, 2),
                functools.partial(last, 2),
            )
        ):
            k = n - late
            pl.when(jnp.logical_and(k >= 0, k < chunks))(functools.partial(work, k))

        @pl.when(n < steps - 2)
        def _():
            for axis in range(3):
                for s in range(2):
                    pl.semaphore_signal(credit.at[2 * axis + 1 - s], inc=1, device_id=here.peer(axis, (1, -1)[s]), device_id_type=MESH)

    for p in range(3):
        for k in range(chunks - SLOTS, chunks):
            for kind in range(3):
                for i in range(3):
                    for s in range(2):
                        message(p, k, i, s, kind).wait_send()

    for axis in range(3):
        mine = here.coords[axis]
        norms[axis, mine] = acc[...]
        copies = [
            pltpu.make_async_remote_copy(
                norms.at[axis, mine],
                norms.at[axis, mine],
                norm_sent.at[axis, offset],
                norm_got.at[axis, offset],
                device_id=here.peer(axis, offset + 1),
                device_id_type=MESH,
            )
            for offset in range(3)
        ]
        for copy in copies:
            copy.start()
        for copy in copies:
            copy.wait()
        acc[...] = norms[axis, 0] + norms[axis, 1] + norms[axis, 2] + norms[axis, 3]

    for load in loads:
        load.wait()
    mean = jnp.sum(acc[...], axis=(0, 1), keepdims=True) / (own.size * RING**3)
    factor = jnp.minimum(1.0, 0.5 * lax.rsqrt(mean + 1e-30))
    for i in range(3):
        for half in range(2):

            @pl.loop(0, total.shape[2] // 8)
            def _(j):
                at = (i, half, pl.ds(j * 8, 8))
                g = total[at].astype(jnp.float32) * factor
                new[at], moments[0][at], moments[1][at] = adamw(own[at].astype(jnp.float32), moments[0][at], moments[1][at], g)


def sum_and_step(terms, weights, m, v, chunks):
    count = terms[0].shape[4]
    tiles = count // chunks
    dma, bf16, f32 = pltpu.SemaphoreType.DMA, jnp.bfloat16, jnp.float32
    subs = ((RING, RING), (RING,), ())
    block = (3, 2, count, 8, 128)
    tile = (tiles, 8, 128)
    per = range(3)
    buffers = (
        pltpu.VMEM((3, STAGES, 2, RING, RING, RING, *tile), bf16),
        [pltpu.VMEM((3, 2, 3, SLOTS, *subs[p], *tile), bf16) for p in per],
        [pltpu.VMEM((3, 2, SLOTS, *subs[p], *tile), bf16) for p in per],
        [pltpu.VMEM((3, 2, 2, SLOTS, *subs[p], *tile) if p else (8, 128), bf16) for p in per],
        [pltpu.VMEM((3, 4, SLOTS, *subs[p], *tile) if p else (8, 128), f32) for p in per],
        pltpu.VMEM(block, bf16),
        pltpu.VMEM(block, bf16),
        pltpu.VMEM((8, 128), f32),
        pltpu.VMEM((3, RING, 8, 128), f32),
    )
    semaphores = (
        dma((3, 3, 2, 3, SLOTS)),
        dma((3, 3, 2, 3, SLOTS)),
        dma((3, STAGES)),
        pltpu.SemaphoreType.REGULAR((6,)),
        dma((3, 3)),
        dma((3, 3)),
        dma((3, 3)),
    )
    return pl.pallas_call(
        functools.partial(sum_kernel, chunks, tiles),
        out_shape=(pltpu.VMEM(block, bf16), pltpu.VMEM(block, f32), pltpu.VMEM(block, f32)),
        in_specs=[pl.BlockSpec(memory_space=pl.ANY)] * 12,
        out_specs=[pl.BlockSpec(memory_space=pltpu.VMEM)] * 3,
        scratch_shapes=[buffers, semaphores],
        compiler_params=pltpu.CompilerParams(collective_id=0, has_side_effects=True, vmem_limit_bytes=48 * 2**20),
        name="sum_and_step",
    )(*terms, *weights, *m, *v)


def gather_kernel(chunks, tiles, *refs):
    blocks, wholes, (sent, got) = [refs[0].at[i] for i in range(3)], [refs[1].at[i] for i in range(3)], refs[2:]
    here = Here()
    here.meet((1, -1))

    def region(i, q, half, offset, k):
        index = list(here.coords)
        for done in range(q):
            index[ORDERS[i][2 - done]] = slice(None)
        axis = ORDERS[i][2 - q]
        index[axis] = here.coord(axis, offset)
        return wholes[i].at[(half, *index, pl.ds(k * tiles, tiles))]

    def message(q, k, i, s, on):
        if on:
            target = region(i, q, s, (-1, 1)[s], k)
        else:
            target = region(i, q, slice(None), 0, k)
        return pltpu.make_async_remote_copy(
            blocks[i].at[:, pl.ds(k * tiles, tiles)] if q == 0 and not on else target,
            target,
            sent.at[q, i, s, on, k],
            got.at[q, i, s, on, k],
            device_id=here.peer(ORDERS[i][2 - q], (1, -1)[s]),
            device_id_type=MESH,
        )

    def each(q, k, on, act):
        for i in range(3):
            for s in range(2):
                act(message(q, k, i, s, on))

    def start(copy):
        copy.start()

    def arrive(copy):
        copy.wait_recv()

    def leave(copy):
        copy.wait_send()

    pl.loop(0, chunks)(lambda k: each(0, k, 0, start))

    @pl.loop(0, chunks)
    def _(k):
        for i in range(3):
            for half in range(2):
                some = pl.ds(k * tiles, tiles)
                wholes[i][(half, *here.coords, some)] = blocks[i][half, some]

    def onward(q, k):
        each(q, k, 0, arrive)
        each(q, k, 1, start)

    def widen(q, k):
        each(q, k, 1, arrive)
        if q < 2:
            each(q + 1, k, 0, start)

    @pl.loop(0, chunks + 5)
    def _(n):
        for late in range(6):
            k = n - late
            work = functools.partial(widen if late % 2 else onward, late // 2, k)
            pl.when(jnp.logical_and(k >= 0, k < chunks))(work)

    @pl.loop(0, chunks)
    def _(k):
        for q in range(3):
            for on in range(2):
                each(q, k, on, leave)


def write_kernel(*refs):
    (wholes, *moments), outs, done = refs[:3], refs[3:12], refs[12]
    copies = [(wholes.at[i, half, x], outs[i].at[half, x]) for i in range(3) for half in range(2) for x in range(RING)]
    copies += [(moments[which].at[i], outs[3 + 3 * which + i]) for which in range(2) for i in range(3)]
    copies = [pltpu.make_async_copy(*copy, done.at[n]) for n, copy in enumerate(copies)]
    for copy in copies:
        copy.start()
    for copy in copies:
        copy.wait()


def gather_and_write(blocks, m, v, chunks):
    count = blocks.shape[2]
    tiles = count // chunks
    dma = pltpu.SemaphoreType.DMA
    shape = (2, RING, RING, RING, count, 8, 128)
    whole = pl.pallas_call(
        functools.partial(gather_kernel, chunks, tiles),
        out_shape=pltpu.VMEM((3, *shape), jnp.bfloat16),
        in_specs=[pl.BlockSpec(memory_space=pltpu.VMEM)],
        out_specs=pl.BlockSpec(memory_space=pltpu.VMEM),
        scratch_shapes=[dma((3, 3, 2, 2, chunks)), dma((3, 3, 2, 2, chunks))],
        compiler_params=pltpu.CompilerParams(collective_id=1, has_side_effects=True, vmem_limit_bytes=2**20),
        name="gather",
    )(blocks)
    return pl.pallas_call(
        write_kernel,
        out_shape=(jax.ShapeDtypeStruct(shape, jnp.bfloat16),) * 3 + (jax.ShapeDtypeStruct(m.shape[1:], jnp.float32),) * 6,
        in_specs=[pl.BlockSpec(memory_space=pltpu.VMEM)] * 3,
        out_specs=[pl.BlockSpec(memory_space=pl.ANY)] * 9,
        scratch_shapes=[dma((30,))],
        compiler_params=pltpu.CompilerParams(has_side_effects=True, vmem_limit_bytes=2**20),
        name="write",
    )(whole, m, v)


def solution(mesh):
    def step(*arrays):
        terms, weights, m, v = (arrays[i : i + 3] for i in (0, 3, 6, 9))
        grid = (2, RING, RING, RING, -1, 8, 128)
        terms = [tiles_of(t[0]).reshape(grid) for t in terms]
        weights = [tiles_of(w).reshape(grid) for w in weights]
        new = sum_and_step(terms, weights, *([tiles_of(one) for one in moment] for moment in (m, v)), 16)
        done = gather_and_write(*new, 8)
        shapes = [one.shape for one in arrays[3:]]
        return tuple(from_tiles(one.reshape(2, -1, 8, 128), *shape[1:]) for one, shape in zip(done, shapes, strict=True))

    all_of, cut = P(None, None, None), P(None, "dp", None)
    return jax.shard_map(
        step,
        mesh=mesh,
        in_specs=(P(("rep", "dp"), None, None, None),) * 3 + (all_of,) * 3 + (cut,) * 6,
        out_specs=(P("rep", None, None),) * 3 + (P("rep", "dp", None),) * 6,
        check_vma=False,
    )
```

```python
import functools

import jax
import jax.numpy as jnp
from jax import lax
from jax.experimental import pallas as pl
from jax.experimental.pallas import tpu as pltpu
from jax.sharding import PartitionSpec as P

MESH = pl.DeviceIdType.MESH
RING = 4
STRIDE = (16, 4, 1)
ORDERS = ((0, 1, 2), (1, 2, 0), (2, 0, 1))
SLOTS = 5
STAGES = 6
CHUNKS = 16
LATE = 28_000
FAR, NEAR, SUM = 0, 1, 2
KEEP_UP, KEEP_DOWN, OWN = 0, 1, 2


def adamw(w, m, v, g):
    m = 0.9 * m + 0.1 * g
    v = 0.95 * v + 0.05 * g * g
    step = m * lax.rsqrt(v + 1e-8) + 0.1 * w
    return (w - 0.02 * step).astype(jnp.bfloat16), m, v


def tiles_of(a):
    layers, rows, columns = a.shape
    a = a.reshape(layers, rows // 8, 8, columns // 128, 128).transpose(0, 1, 3, 2, 4)
    return a.reshape(layers, rows // 8 * columns // 128, 8, 128)


def from_tiles(a, rows, columns):
    a = a.reshape(a.shape[0], rows // 8, columns // 128, 8, 128).transpose(0, 1, 3, 2, 4)
    return a.reshape(a.shape[0], rows, columns)


class Here:
    def __init__(self):
        self.index = lax.axis_index("dp")
        self.coords = tuple(lax.rem(lax.div(self.index, stride), RING) for stride in STRIDE)

    def coord(self, axis, offset):
        return lax.rem(self.coords[axis] + (offset + RING), RING)

    def peer(self, axis, offset):
        return {"dp": self.index + (self.coord(axis, offset) - self.coords[axis]) * STRIDE[axis]}

    def meet(self, offsets):
        barrier = pltpu.get_barrier_semaphore()
        for axis in range(3):
            for offset in offsets:
                pl.semaphore_signal(barrier, inc=1, device_id=self.peer(axis, offset), device_id_type=MESH)
        pl.semaphore_wait(barrier, 3 * len(offsets))


def sum_kernel(chunks, tiles, *refs):
    terms, weights, old, (new, *moments), scratch = refs[:3], refs[3:6], refs[6:12], refs[12:15], refs[15:]
    (stage, recv, sums, outs, keep, total, own, acc, norms), (sent, got, staged, credit, norm_sent, norm_got, loaded) = scratch
    here = Here()
    steps = chunks + 7

    def part(i, half, offset, k, rest):
        axis = ORDERS[i][0]
        index = (*rest[:axis], here.coord(axis, offset), *rest[axis:])
        return (i, lax.rem(k, STAGES), half, *index)

    everything = (slice(None),) * 2

    def message(p, k, i, s, kind):
        axis, slot = ORDERS[i][p], lax.rem(k, SLOTS)
        if kind == SUM:
            source = sums[p].at[i, s, slot]
        elif p:
            source = outs[p].at[i, s, kind, slot]
        elif kind == FAR:
            source = stage.at[part(i, s, 2, k, everything)]
        else:
            source = stage.at[part(i, 1 - s, (1, -1)[s], k, everything)]
        return pltpu.make_async_remote_copy(
            source,
            recv[p].at[i, s, kind, slot],
            sent.at[p, i, s, kind, slot],
            got.at[p, i, s, kind, slot],
            device_id=here.peer(axis, (1, -1)[s]),
            device_id_type=MESH,
        )

    def staging(k, i):
        slot = lax.rem(k, STAGES)
        source = terms[i].at[:, :, :, :, pl.ds(k * tiles, tiles)]
        return pltpu.make_async_copy(source, stage.at[i, slot], staged.at[i, slot])

    loads = []
    for i in range(3):
        loads.append(pltpu.make_async_copy(weights[i].at[(slice(None), *here.coords)], own.at[i], loaded.at[i, 0]))
        for which in range(2):
            loads.append(pltpu.make_async_copy(old[3 * which + i], moments[which].at[i], loaded.at[i, 1 + which]))
    for i in range(3):
        staging(0, i).start()
    for load in loads:
        load.start()
    here.meet((1, -1, 2))
    pl.when(lax.axis_index("rep") == 1)(lambda: pl.delay(LATE))

    def start(p, k, kinds):
        for kind in kinds:
            for i in range(3):
                for s in range(2):
                    message(p, k, i, s, kind).start()

    def reuse(p, k, kinds):
        @pl.when(k >= SLOTS)
        def _():
            for kind in kinds:
                for i in range(3):
                    for s in range(2):
                        message(p, k - SLOTS, i, s, kind).wait_send()

    def first(k):
        reuse(0, k, (FAR, NEAR))
        for i in range(3):
            staging(k, i).wait()
        start(0, k, (FAR, NEAR))

        @pl.when(k + 1 < chunks)
        def _():
            for i in range(3):
                staging(k + 1, i).start()

    def held(p, i, what, k, index):
        if p:
            return keep[p][(i, what, lax.rem(k, SLOTS), *index)]
        half, offset = ((0, 1), (1, -1), (0, 0), (1, 0))[what]
        return stage[part(i, half, offset, k, index)].astype(jnp.float32)

    def middle(p, k):
        slot = lax.rem(k, SLOTS)
        reuse(p, k, (SUM,))
        for i in range(3):
            for s in range(2):
                message(p, k, i, s, FAR).wait_recv()

                def add(index):
                    whole = held(p, i, s, k, index) + recv[p][(i, s, FAR, slot, *index)].astype(jnp.float32)
                    sums[p][(i, s, slot, *index)] = whole.astype(jnp.bfloat16)

                if p == 0:
                    pl.loop(0, RING * RING)(lambda j: add((lax.div(j, RING), lax.rem(j, RING))))
                elif p == 1:
                    pl.loop(0, RING)(lambda j: add((j,)))
                else:
                    add(())
        start(p, k, (SUM,))

    def last(p, k):
        slot = lax.rem(k, SLOTS)
        if p < 2:
            reuse(p + 1, k, (FAR, NEAR))
        for i in range(3):
            for s in range(2):
                message(p, k, i, s, SUM).wait_recv()
                message(p, k, i, s, NEAR).wait_recv()

            def whole(half, index):
                return (
                    held(p, i, OWN + half, k, index)
                    + recv[p][(i, half, SUM, slot, *index)].astype(jnp.float32)
                    + recv[p][(i, 1 - half, NEAR, slot, *index)].astype(jnp.float32)
                )

            if p == 2:
                for half in range(2):
                    g = whole(half, ()).astype(jnp.bfloat16)
                    total[i, half, pl.ds(k * tiles, tiles)] = g
                    g = g.astype(jnp.float32)
                    acc[...] += jnp.sum(g * g, axis=0)
                continue
            axis = ORDERS[i][p + 1]

            def pass_on(below):
                for half in range(2):
                    for offset in range(RING):
                        at = here.coord(axis, offset)
                        if p == 1:
                            index = (at,)
                        elif axis > ORDERS[i][2]:
                            index = (below, at)
                        else:
                            index = (at, below)
                        value = whole(half, index)
                        to = () if p == 1 else (below,)
                        if offset == 0:
                            keep[p + 1][(i, OWN + half, slot, *to)] = value
                        elif offset == (1, 3)[half]:
                            keep[p + 1][(i, half, slot, *to)] = value
                        elif offset == 2:
                            outs[p + 1][(i, half, FAR, slot, *to)] = value.astype(jnp.bfloat16)
                        else:
                            outs[p + 1][(i, 1 - half, NEAR, slot, *to)] = value.astype(jnp.bfloat16)

            if p == 0:
                pl.loop(0, RING)(pass_on)
            else:
                pass_on(None)
        if p < 2:
            start(p + 1, k, (FAR, NEAR))

    acc[...] = jnp.zeros_like(acc)

    @pl.loop(0, steps)
    def _(n):
        @pl.when(n >= 2)
        def _():
            for to in range(6):
                pl.semaphore_wait(credit.at[to], 1)

        for late, work in (
            (0, first),
            (2, functools.partial(middle, 0)),
            (3, functools.partial(last, 0)),
            (4, functools.partial(middle, 1)),
            (5, functools.partial(last, 1)),
            (6, functools.partial(middle, 2)),
            (7, functools.partial(last, 2)),
        ):
            k = n - late
            pl.when(jnp.logical_and(k >= 0, k < chunks))(functools.partial(work, k))

        @pl.when(n < steps - 2)
        def _():
            for axis in range(3):
                for s in range(2):
                    pl.semaphore_signal(credit.at[2 * axis + 1 - s], inc=1, device_id=here.peer(axis, (1, -1)[s]), device_id_type=MESH)

    for p in range(3):
        for k in range(chunks - SLOTS, chunks):
            for kind in range(3):
                for i in range(3):
                    for s in range(2):
                        message(p, k, i, s, kind).wait_send()

    for axis in range(3):
        mine = here.coords[axis]
        norms[axis, mine] = acc[...]
        copies = [
            pltpu.make_async_remote_copy(
                norms.at[axis, mine],
                norms.at[axis, mine],
                norm_sent.at[axis, offset],
                norm_got.at[axis, offset],
                device_id=here.peer(axis, offset + 1),
                device_id_type=MESH,
            )
            for offset in range(3)
        ]
        for copy in copies:
            copy.start()
        for copy in copies:
            copy.wait()
        acc[...] = norms[axis, 0] + norms[axis, 1] + norms[axis, 2] + norms[axis, 3]

    for load in loads:
        load.wait()
    mean = jnp.sum(acc[...], axis=(0, 1), keepdims=True) / (own.size * RING**3)
    factor = jnp.minimum(1.0, 0.5 * lax.rsqrt(mean + 1e-30))
    for i in range(3):
        for half in range(2):

            @pl.loop(0, total.shape[2] // 8)
            def _(j):
                at = (i, half, pl.ds(j * 8, 8))
                g = total[at].astype(jnp.float32) * factor
                new[at], moments[0][at], moments[1][at] = adamw(own[at].astype(jnp.float32), moments[0][at], moments[1][at], g)


def sum_and_step(terms, weights, m, v, chunks):
    count = terms[0].shape[4]
    tiles = count // chunks
    dma, bf16, f32 = pltpu.SemaphoreType.DMA, jnp.bfloat16, jnp.float32
    subs = ((RING, RING), (RING,), ())
    block = (3, 2, count, 8, 128)
    tile = (tiles, 8, 128)
    per = range(3)
    buffers = (
        pltpu.VMEM((3, STAGES, 2, RING, RING, RING, *tile), bf16),
        [pltpu.VMEM((3, 2, 3, SLOTS, *subs[p], *tile), bf16) for p in per],
        [pltpu.VMEM((3, 2, SLOTS, *subs[p], *tile), bf16) for p in per],
        [pltpu.VMEM((3, 2, 2, SLOTS, *subs[p], *tile) if p else (8, 128), bf16) for p in per],
        [pltpu.VMEM((3, 4, SLOTS, *subs[p], *tile) if p else (8, 128), f32) for p in per],
        pltpu.VMEM(block, bf16),
        pltpu.VMEM(block, bf16),
        pltpu.VMEM((8, 128), f32),
        pltpu.VMEM((3, RING, 8, 128), f32),
    )
    semaphores = (
        dma((3, 3, 2, 3, SLOTS)),
        dma((3, 3, 2, 3, SLOTS)),
        dma((3, STAGES)),
        pltpu.SemaphoreType.REGULAR((6,)),
        dma((3, 3)),
        dma((3, 3)),
        dma((3, 3)),
    )
    return pl.pallas_call(
        functools.partial(sum_kernel, chunks, tiles),
        out_shape=(pltpu.VMEM(block, bf16), pltpu.VMEM(block, f32), pltpu.VMEM(block, f32)),
        in_specs=[pl.BlockSpec(memory_space=pltpu.HBM)] * 12,
        out_specs=[pl.BlockSpec(memory_space=pltpu.VMEM)] * 3,
        scratch_shapes=[buffers, semaphores],
        compiler_params=pltpu.CompilerParams(collective_id=0, has_side_effects=True, vmem_limit_bytes=60 * 2**20),
        name="sum_and_step",
    )(*terms, *weights, *m, *v)


def gather_kernel(chunks, tiles, *refs):
    blocks, wholes, (sent, got) = [refs[0].at[i] for i in range(3)], [refs[1].at[i] for i in range(3)], refs[2:]
    here = Here()
    here.meet((1, -1))

    def region(i, q, half, offset, k):
        index = list(here.coords)
        for done in range(q):
            index[ORDERS[i][2 - done]] = slice(None)
        axis = ORDERS[i][2 - q]
        index[axis] = here.coord(axis, offset)
        return wholes[i].at[(half, *index, pl.ds(k * tiles, tiles))]

    def message(q, k, i, s, on):
        if on:
            target = region(i, q, s, (-1, 1)[s], k)
        else:
            target = region(i, q, slice(None), 0, k)
        return pltpu.make_async_remote_copy(
            blocks[i].at[:, pl.ds(k * tiles, tiles)] if q == 0 and not on else target,
            target,
            sent.at[q, i, s, on, k],
            got.at[q, i, s, on, k],
            device_id=here.peer(ORDERS[i][2 - q], (1, -1)[s]),
            device_id_type=MESH,
        )

    def each(q, k, on, act):
        for i in range(3):
            for s in range(2):
                act(message(q, k, i, s, on))

    def start(copy):
        copy.start()

    def arrive(copy):
        copy.wait_recv()

    def leave(copy):
        copy.wait_send()

    pl.loop(0, chunks)(lambda k: each(0, k, 0, start))

    @pl.loop(0, chunks)
    def _(k):
        for i in range(3):
            for half in range(2):
                some = pl.ds(k * tiles, tiles)
                wholes[i][(half, *here.coords, some)] = blocks[i][half, some]

    def onward(q, k):
        each(q, k, 0, arrive)
        each(q, k, 1, start)

    def widen(q, k):
        each(q, k, 1, arrive)
        if q < 2:
            each(q + 1, k, 0, start)

    @pl.loop(0, chunks + 6)
    def _(n):
        for stage, late in enumerate((0, 1, 2, 3, 5, 6)):
            k = n - late
            work = functools.partial(widen if stage % 2 else onward, stage // 2, k)
            pl.when(jnp.logical_and(k >= 0, k < chunks))(work)

    @pl.loop(0, chunks)
    def _(k):
        for q in range(3):
            for on in range(2):
                each(q, k, on, leave)


def write_kernel(*refs):
    (wholes, *moments), outs, done = refs[:3], refs[3:12], refs[12]
    copies = [(wholes.at[i, half, x], outs[i].at[half, x]) for i in range(3) for half in range(2) for x in range(RING)]
    copies += [(moments[which].at[i], outs[3 + 3 * which + i]) for which in range(2) for i in range(3)]
    copies = [pltpu.make_async_copy(*copy, done.at[n]) for n, copy in enumerate(copies)]
    for copy in copies:
        copy.start()
    for copy in copies:
        copy.wait()


def gather_and_write(blocks, m, v, chunks):
    count = blocks.shape[2]
    tiles = count // chunks
    dma = pltpu.SemaphoreType.DMA
    shape = (2, RING, RING, RING, count, 8, 128)
    whole = pl.pallas_call(
        functools.partial(gather_kernel, chunks, tiles),
        out_shape=pltpu.VMEM((3, *shape), jnp.bfloat16),
        in_specs=[pl.BlockSpec(memory_space=pltpu.VMEM)],
        out_specs=pl.BlockSpec(memory_space=pltpu.VMEM),
        scratch_shapes=[dma((3, 3, 2, 2, chunks)), dma((3, 3, 2, 2, chunks))],
        compiler_params=pltpu.CompilerParams(collective_id=1, has_side_effects=True, vmem_limit_bytes=2**20),
        name="gather",
    )(blocks)
    return pl.pallas_call(
        write_kernel,
        out_shape=(jax.ShapeDtypeStruct(shape, jnp.bfloat16),) * 3 + (jax.ShapeDtypeStruct(m.shape[1:], jnp.float32),) * 6,
        in_specs=[pl.BlockSpec(memory_space=pltpu.VMEM)] * 3,
        out_specs=[pl.BlockSpec(memory_space=pl.ANY)] * 9,
        scratch_shapes=[dma((30,))],
        compiler_params=pltpu.CompilerParams(has_side_effects=True, vmem_limit_bytes=2**20),
        name="write",
    )(whole, m, v)


def solution(mesh):
    def step(*arrays):
        terms, weights, m, v = (arrays[i : i + 3] for i in (0, 3, 6, 9))
        grid = (2, RING, RING, RING, -1, 8, 128)
        terms = [tiles_of(t[0]).reshape(grid) for t in terms]
        weights = [tiles_of(w).reshape(grid) for w in weights]
        new = sum_and_step(terms, weights, *([tiles_of(one) for one in moment] for moment in (m, v)), CHUNKS)
        done = gather_and_write(*new, 8)
        shapes = [one.shape for one in arrays[3:]]
        return tuple(from_tiles(one.reshape(2, -1, 8, 128), *shape[1:]) for one, shape in zip(done, shapes, strict=True))

    all_of, cut = P(None, None, None), P(None, "dp", None)
    return jax.shard_map(
        step,
        mesh=mesh,
        in_specs=(P(("rep", "dp"), None, None, None),) * 3 + (all_of,) * 3 + (cut,) * 6,
        out_specs=(P("rep", None, None),) * 3 + (P("rep", "dp", None),) * 6,
        check_vma=False,
    )
```

```python
import functools

import jax
import jax.numpy as jnp
from jax import lax
from jax.experimental import pallas as pl
from jax.experimental.pallas import tpu as pltpu
from jax.sharding import PartitionSpec as P

MESH = pl.DeviceIdType.MESH
RING = 4
STRIDE = (16, 4, 1)
ORDERS = ((0, 1, 2), (1, 2, 0), (2, 0, 1))
SLOTS = 4
STAGES = 5
CHUNKS = 16
LATE = 30_000
FAR, NEAR, SUM = 0, 1, 2
KEEP_UP, KEEP_DOWN, OWN = 0, 1, 2


def adamw(w, m, v, g):
    m = 0.9 * m + 0.1 * g
    v = 0.95 * v + 0.05 * g * g
    step = m * lax.rsqrt(v + 1e-8) + 0.1 * w
    return (w - 0.02 * step).astype(jnp.bfloat16), m, v


def tiles_of(a):
    layers, rows, columns = a.shape
    a = a.reshape(layers, rows // 8, 8, columns // 128, 128).transpose(0, 1, 3, 2, 4)
    return a.reshape(layers, rows // 8 * columns // 128, 8, 128)


def from_tiles(a, rows, columns):
    a = a.reshape(a.shape[0], rows // 8, columns // 128, 8, 128).transpose(0, 1, 3, 2, 4)
    return a.reshape(a.shape[0], rows, columns)


class Here:
    def __init__(self):
        self.index = lax.axis_index("dp")
        self.coords = tuple(lax.rem(lax.div(self.index, stride), RING) for stride in STRIDE)

    def coord(self, axis, offset):
        return lax.rem(self.coords[axis] + (offset + RING), RING)

    def peer(self, axis, offset):
        return {"dp": self.index + (self.coord(axis, offset) - self.coords[axis]) * STRIDE[axis]}

    def meet(self, offsets):
        barrier = pltpu.get_barrier_semaphore()
        for axis in range(3):
            for offset in offsets:
                pl.semaphore_signal(barrier, inc=1, device_id=self.peer(axis, offset), device_id_type=MESH)
        pl.semaphore_wait(barrier, 3 * len(offsets))


def sum_kernel(chunks, tiles, *refs):
    terms, weights, old, (new, *moments), scratch = refs[:3], refs[3:6], refs[6:12], refs[12:15], refs[15:]
    (stage, recv, sums, outs, keep, total, own, acc, norms), (sent, got, staged, credit, norm_sent, norm_got, loaded) = scratch
    here = Here()
    steps = chunks + 6

    def part(i, half, offset, k, rest):
        axis = ORDERS[i][0]
        index = (*rest[:axis], here.coord(axis, offset), *rest[axis:])
        return (i, lax.rem(k, STAGES), half, *index)

    everything = (slice(None),) * 2

    def message(p, k, i, s, kind):
        axis, slot = ORDERS[i][p], lax.rem(k, SLOTS)
        if kind == SUM:
            source = sums[p].at[i, s, slot]
        elif p:
            source = outs[p].at[i, s, kind, slot]
        elif kind == FAR:
            source = stage.at[part(i, s, 2, k, everything)]
        else:
            source = stage.at[part(i, 1 - s, (1, -1)[s], k, everything)]
        return pltpu.make_async_remote_copy(
            source,
            recv[p].at[i, s, kind, slot],
            sent.at[p, i, s, kind, slot],
            got.at[p, i, s, kind, slot],
            device_id=here.peer(axis, (1, -1)[s]),
            device_id_type=MESH,
        )

    def staging(k, i):
        slot = lax.rem(k, STAGES)
        source = terms[i].at[:, :, :, :, pl.ds(k * tiles, tiles)]
        return pltpu.make_async_copy(source, stage.at[i, slot], staged.at[i, slot])

    loads = []
    for i in range(3):
        loads.append(pltpu.make_async_copy(weights[i].at[(slice(None), *here.coords)], own.at[i], loaded.at[i, 0]))
        for which in range(2):
            loads.append(pltpu.make_async_copy(old[3 * which + i], moments[which].at[i], loaded.at[i, 1 + which]))
    for i in range(3):
        staging(0, i).start()
    for load in loads:
        load.start()
    here.meet((1, -1, 2))
    pl.when(lax.axis_index("rep") == 1)(lambda: pl.delay(LATE))

    def start(p, k, kinds):
        for kind in kinds:
            for i in range(3):
                for s in range(2):
                    message(p, k, i, s, kind).start()

    def reuse(p, k, kinds):
        @pl.when(k >= SLOTS)
        def _():
            for kind in kinds:
                for i in range(3):
                    for s in range(2):
                        message(p, k - SLOTS, i, s, kind).wait_send()

    def first(k):
        reuse(0, k, (FAR, NEAR))
        for i in range(3):
            staging(k, i).wait()
        start(0, k, (FAR, NEAR))

        @pl.when(k + 1 < chunks)
        def _():
            for i in range(3):
                staging(k + 1, i).start()

    def held(p, i, what, k, index):
        if p:
            return keep[p][(i, what, lax.rem(k, SLOTS), *index)]
        half, offset = ((0, 1), (1, -1), (0, 0), (1, 0))[what]
        return stage[part(i, half, offset, k, index)].astype(jnp.float32)

    def middle(p, k):
        slot = lax.rem(k, SLOTS)
        reuse(p, k, (SUM,))
        for i in range(3):
            for s in range(2):
                message(p, k, i, s, FAR).wait_recv()

                def add(index):
                    whole = held(p, i, s, k, index) + recv[p][(i, s, FAR, slot, *index)].astype(jnp.float32)
                    sums[p][(i, s, slot, *index)] = whole.astype(jnp.bfloat16)

                if p == 0:
                    pl.loop(0, RING * RING)(lambda j: add((lax.div(j, RING), lax.rem(j, RING))))
                elif p == 1:
                    pl.loop(0, RING)(lambda j: add((j,)))
                else:
                    add(())
        start(p, k, (SUM,))

    def last(p, k):
        slot = lax.rem(k, SLOTS)
        if p < 2:
            reuse(p + 1, k, (FAR, NEAR))
        for i in range(3):
            for s in range(2):
                message(p, k, i, s, SUM).wait_recv()
                message(p, k, i, s, NEAR).wait_recv()

            def whole(half, index):
                return (
                    held(p, i, OWN + half, k, index)
                    + recv[p][(i, half, SUM, slot, *index)].astype(jnp.float32)
                    + recv[p][(i, 1 - half, NEAR, slot, *index)].astype(jnp.float32)
                )

            if p == 2:
                for half in range(2):
                    g = whole(half, ()).astype(jnp.bfloat16)
                    total[i, half, pl.ds(k * tiles, tiles)] = g
                    g = g.astype(jnp.float32)
                    acc[...] += jnp.sum(g * g, axis=0)
                continue
            axis = ORDERS[i][p + 1]

            def pass_on(below):
                for half in range(2):
                    for offset in range(RING):
                        at = here.coord(axis, offset)
                        if p == 1:
                            index = (at,)
                        elif axis > ORDERS[i][2]:
                            index = (below, at)
                        else:
                            index = (at, below)
                        value = whole(half, index)
                        to = () if p == 1 else (below,)
                        if offset == 0:
                            keep[p + 1][(i, OWN + half, slot, *to)] = value
                        elif offset == (1, 3)[half]:
                            keep[p + 1][(i, half, slot, *to)] = value
                        elif offset == 2:
                            outs[p + 1][(i, half, FAR, slot, *to)] = value.astype(jnp.bfloat16)
                        else:
                            outs[p + 1][(i, 1 - half, NEAR, slot, *to)] = value.astype(jnp.bfloat16)

            if p == 0:
                pl.loop(0, RING)(pass_on)
            else:
                pass_on(None)
        if p < 2:
            start(p + 1, k, (FAR, NEAR))

    acc[...] = jnp.zeros_like(acc)

    @pl.loop(0, steps)
    def _(n):
        @pl.when(n >= 2)
        def _():
            for to in range(6):
                pl.semaphore_wait(credit.at[to], 1)

        for late, work in enumerate(
            (
                first,
                functools.partial(middle, 0),
                functools.partial(last, 0),
                functools.partial(middle, 1),
                functools.partial(last, 1),
                functools.partial(middle, 2),
                functools.partial(last, 2),
            )
        ):
            k = n - late
            pl.when(jnp.logical_and(k >= 0, k < chunks))(functools.partial(work, k))

        @pl.when(n < steps - 2)
        def _():
            for axis in range(3):
                for s in range(2):
                    pl.semaphore_signal(credit.at[2 * axis + 1 - s], inc=1, device_id=here.peer(axis, (1, -1)[s]), device_id_type=MESH)

    for p in range(3):
        for k in range(chunks - SLOTS, chunks):
            for kind in range(3):
                for i in range(3):
                    for s in range(2):
                        message(p, k, i, s, kind).wait_send()

    for axis in range(3):
        mine = here.coords[axis]
        norms[axis, mine] = acc[...]
        copies = [
            pltpu.make_async_remote_copy(
                norms.at[axis, mine],
                norms.at[axis, mine],
                norm_sent.at[axis, offset],
                norm_got.at[axis, offset],
                device_id=here.peer(axis, offset + 1),
                device_id_type=MESH,
            )
            for offset in range(3)
        ]
        for copy in copies:
            copy.start()
        for copy in copies:
            copy.wait()
        acc[...] = norms[axis, 0] + norms[axis, 1] + norms[axis, 2] + norms[axis, 3]

    for load in loads:
        load.wait()
    mean = jnp.sum(acc[...], axis=(0, 1), keepdims=True) / (own.size * RING**3)
    factor = jnp.minimum(1.0, 0.5 * lax.rsqrt(mean + 1e-30))
    for i in range(3):
        for half in range(2):

            @pl.loop(0, total.shape[2] // 8)
            def _(j):
                at = (i, half, pl.ds(j * 8, 8))
                g = total[at].astype(jnp.float32) * factor
                new[at], moments[0][at], moments[1][at] = adamw(own[at].astype(jnp.float32), moments[0][at], moments[1][at], g)


def sum_and_step(terms, weights, m, v, chunks):
    count = terms[0].shape[4]
    tiles = count // chunks
    dma, bf16, f32 = pltpu.SemaphoreType.DMA, jnp.bfloat16, jnp.float32
    subs = ((RING, RING), (RING,), ())
    block = (3, 2, count, 8, 128)
    tile = (tiles, 8, 128)
    per = range(3)
    buffers = (
        pltpu.VMEM((3, STAGES, 2, RING, RING, RING, *tile), bf16),
        [pltpu.VMEM((3, 2, 3, SLOTS, *subs[p], *tile), bf16) for p in per],
        [pltpu.VMEM((3, 2, SLOTS, *subs[p], *tile), bf16) for p in per],
        [pltpu.VMEM((3, 2, 2, SLOTS, *subs[p], *tile) if p else (8, 128), bf16) for p in per],
        [pltpu.VMEM((3, 4, SLOTS, *subs[p], *tile) if p else (8, 128), f32) for p in per],
        pltpu.VMEM(block, bf16),
        pltpu.VMEM(block, bf16),
        pltpu.VMEM((8, 128), f32),
        pltpu.VMEM((3, RING, 8, 128), f32),
    )
    semaphores = (
        dma((3, 3, 2, 3, SLOTS)),
        dma((3, 3, 2, 3, SLOTS)),
        dma((3, STAGES)),
        pltpu.SemaphoreType.REGULAR((6,)),
        dma((3, 3)),
        dma((3, 3)),
        dma((3, 3)),
    )
    return pl.pallas_call(
        functools.partial(sum_kernel, chunks, tiles),
        out_shape=(pltpu.VMEM(block, bf16), pltpu.VMEM(block, f32), pltpu.VMEM(block, f32)),
        in_specs=[pl.BlockSpec(memory_space=pltpu.HBM)] * 12,
        out_specs=[pl.BlockSpec(memory_space=pltpu.VMEM)] * 3,
        scratch_shapes=[buffers, semaphores],
        compiler_params=pltpu.CompilerParams(collective_id=0, has_side_effects=True, vmem_limit_bytes=60 * 2**20),
        name="sum_and_step",
    )(*terms, *weights, *m, *v)


def gather_kernel(chunks, tiles, *refs):
    blocks, wholes, (sent, got) = [refs[0].at[i] for i in range(3)], [refs[1].at[i] for i in range(3)], refs[2:]
    here = Here()
    here.meet((1, -1))

    def region(i, q, half, offset, k):
        index = list(here.coords)
        for done in range(q):
            index[ORDERS[i][2 - done]] = slice(None)
        axis = ORDERS[i][2 - q]
        index[axis] = here.coord(axis, offset)
        return wholes[i].at[(half, *index, pl.ds(k * tiles, tiles))]

    def message(q, k, i, s, on):
        if on:
            target = region(i, q, s, (-1, 1)[s], k)
        else:
            target = region(i, q, slice(None), 0, k)
        return pltpu.make_async_remote_copy(
            blocks[i].at[:, pl.ds(k * tiles, tiles)] if q == 0 and not on else target,
            target,
            sent.at[q, i, s, on, k],
            got.at[q, i, s, on, k],
            device_id=here.peer(ORDERS[i][2 - q], (1, -1)[s]),
            device_id_type=MESH,
        )

    def each(q, k, on, act):
        for i in range(3):
            for s in range(2):
                act(message(q, k, i, s, on))

    def start(copy):
        copy.start()

    def arrive(copy):
        copy.wait_recv()

    def leave(copy):
        copy.wait_send()

    pl.loop(0, 2)(lambda k: each(0, k, 0, start))

    @pl.loop(0, chunks)
    def _(k):
        for i in range(3):
            for half in range(2):
                some = pl.ds(k * tiles, tiles)
                wholes[i][(half, *here.coords, some)] = blocks[i][half, some]

    def onward(q, k):
        each(q, k, 0, arrive)
        each(q, k, 1, start)

    def widen(q, k):
        each(q, k, 1, arrive)
        if q < 2:
            each(q + 1, k, 0, start)

    @pl.loop(0, chunks + 6)
    def _(n):
        pl.when(n + 2 < chunks)(lambda: each(0, n + 2, 0, start))
        for stage, late in enumerate((0, 1, 2, 3, 5, 6)):
            k = n - late
            work = functools.partial(widen if stage % 2 else onward, stage // 2, k)
            pl.when(jnp.logical_and(k >= 0, k < chunks))(work)

    @pl.loop(0, chunks)
    def _(k):
        for q in range(3):
            for on in range(2):
                each(q, k, on, leave)


def write_kernel(*refs):
    (wholes, *moments), outs, done = refs[:3], refs[3:12], refs[12]
    copies = [(wholes.at[i, half, x], outs[i].at[half, x]) for i in range(3) for half in range(2) for x in range(RING)]
    copies += [(moments[which].at[i], outs[3 + 3 * which + i]) for which in range(2) for i in range(3)]
    copies = [pltpu.make_async_copy(*copy, done.at[n]) for n, copy in enumerate(copies)]
    for copy in copies:
        copy.start()
    for copy in copies:
        copy.wait()


def gather_and_write(blocks, m, v, chunks):
    count = blocks.shape[2]
    tiles = count // chunks
    dma = pltpu.SemaphoreType.DMA
    shape = (2, RING, RING, RING, count, 8, 128)
    whole = pl.pallas_call(
        functools.partial(gather_kernel, chunks, tiles),
        out_shape=pltpu.VMEM((3, *shape), jnp.bfloat16),
        in_specs=[pl.BlockSpec(memory_space=pltpu.VMEM)],
        out_specs=pl.BlockSpec(memory_space=pltpu.VMEM),
        scratch_shapes=[dma((3, 3, 2, 2, chunks)), dma((3, 3, 2, 2, chunks))],
        compiler_params=pltpu.CompilerParams(collective_id=1, has_side_effects=True, vmem_limit_bytes=2**20),
        name="gather",
    )(blocks)
    return pl.pallas_call(
        write_kernel,
        out_shape=(jax.ShapeDtypeStruct(shape, jnp.bfloat16),) * 3 + (jax.ShapeDtypeStruct(m.shape[1:], jnp.float32),) * 6,
        in_specs=[pl.BlockSpec(memory_space=pltpu.VMEM)] * 3,
        out_specs=[pl.BlockSpec(memory_space=pl.ANY)] * 9,
        scratch_shapes=[dma((30,))],
        compiler_params=pltpu.CompilerParams(has_side_effects=True, vmem_limit_bytes=2**20),
        name="write",
    )(whole, m, v)


def solution(mesh):
    def step(*arrays):
        terms, weights, m, v = (arrays[i : i + 3] for i in (0, 3, 6, 9))
        grid = (2, RING, RING, RING, -1, 8, 128)
        terms = [tiles_of(t[0]).reshape(grid) for t in terms]
        weights = [tiles_of(w).reshape(grid) for w in weights]
        new = sum_and_step(terms, weights, *([tiles_of(one) for one in moment] for moment in (m, v)), CHUNKS)
        done = gather_and_write(*new, 8)
        shapes = [one.shape for one in arrays[3:]]
        return tuple(from_tiles(one.reshape(2, -1, 8, 128), *shape[1:]) for one, shape in zip(done, shapes, strict=True))

    all_of, cut = P(None, None, None), P(None, "dp", None)
    return jax.shard_map(
        step,
        mesh=mesh,
        in_specs=(P(("rep", "dp"), None, None, None),) * 3 + (all_of,) * 3 + (cut,) * 6,
        out_specs=(P("rep", None, None),) * 3 + (P("rep", "dp", None),) * 6,
        check_vma=False,
    )
```
